32 devices in a mesh: member: 2 (over y), lon: 4 (over z), lat: 4 (over x, core).
Axes of the slice: x: 2, y: 2, z: 4, core: 2. Of those that a mesh axis runs over, the one named last changes fastest.
Arguments:
- tracer: float32 [64, 64, 512], P('member', 'lat', 'lon'), parts along dimension 0, may hold values from -6 to 6
- velocity: float32 [2, 64, 64, 512], P(None, 'member', 'lat', 'lon'), parts along dimension 1, may hold values from -0.9 to 0.9
- surface: float32 [128, 512], P(('member', 'lat'), 'lon'), parts along dimension 0, may hold values from -6 to 6
- transport: float32 [4, 64, 512], P('member', 'lat', 'lon'), parts along dimension 0, may hold values from -3 to 3
- horiz_mixing: float32 [64], P('member'), parts along dimension 0, may hold values from 0.03 to 0.2
- vert_mixing: float32 [62], P('member'), parts along dimension 0, may hold values from 0.3 to 30
- levels: int32 [64, 512], P('lat', 'lon'), may hold values from 0 to 32, as said below
- land_tiles: int32 [4, 4], P('lat', 'lon'), may hold values 0 or 1
- fold_pair: int32 [512], P('lon'), may hold values from 0 to 511, as said below
Outputs:
- tracer_new: float32 [64, 64, 512], P('member', 'lat', 'lon'), parts along dimension 0
- surface_new: float32 [128, 512], P(('member', 'lat'), 'lon'), parts along dimension 0
- transport_new: float32 [4, 64, 512], P('member', 'lat', 'lon'), parts along dimension 0
The draws below stay inside these ranges and needn't reach their ends.
There are 2 independent parts, one for each index of `member`. The reference program is written for one: setup_inputs(seed, part) draws one part's arguments, and reference() takes and returns one part's arrays. A program takes and returns all parts, laid end to end along the dimension named above; an argument that names none is the same for every part. Nothing has to cross between parts.
Inputs may be any that keep to these rules, and one draw needn't show every extreme that they name: 0 marks a land cell, otherwise the count of sea levels. The fold pairing is a reflection: fold_pair[i] = (p - i) mod 512 for one p in 0..4095, so fold_pair[fold_pair[i]] = i.
All inputs are finite; a program needn't handle non-finite values. No bound on the sum of `land_tiles` on one device may be relied on, other than what follows from the above.
Results may differ from the reference program's by a relative error of at most 0.00002.
Values sent between devices are 32-bit elements; how exact they have to be, the bound alone decides.
A program may use at most 64 MiB of HBM per device.

```python
import math
import jax
import jax.numpy as jnp

K = 32
SUB = 12
CLAT = 16
CLON = 128
NLAT = 64
NLON = 512
N_LON = 4
N_LAT = 4


def draw_levels(key, part):
    land_key = jax.random.fold_in(key, 11)
    depth_key = jax.random.fold_in(key, 12)
    land_cells = jax.random.randint(land_key, (NLAT, NLON), 0, 5) == 0
    depth_draw = jax.random.randint(depth_key, (NLAT, NLON), 1, K + 1)
    return jnp.where(land_cells, 0, depth_draw).astype(jnp.int32)


def draw_fold_pair(key, part):
    pivot_key = jax.random.fold_in(key, 21)
    pivot_col = jax.random.randint(pivot_key, (), 0, NLON)
    return jnp.mod(pivot_col - jnp.arange(NLON, dtype=jnp.int32), NLON).astype(jnp.int32)


def set_ends(result, own_key, low, top_value):
    longest = result.shape.index(max(result.shape))
    spots = []
    for shift in (0, 1):
        where = [jax.random.randint(jax.random.fold_in(own_key, axis), (), 0, length) for axis, length in enumerate(result.shape)]
        where[longest] = (where[longest] + shift) % result.shape[longest]
        spots.append(tuple(where))
    return result.at[spots[0]].set(low).at[spots[1]].set(top_value)


def shard_levels(rng, shape, shards, least, top_value):
    loudness = 1.0
    for position, blocks in shards:
        draws = jax.random.uniform(jax.random.fold_in(jax.random.fold_in(rng, 6), position), (blocks,), jnp.float32, least / len(shards), top_value / len(shards))
        loudness = loudness * jnp.repeat(jnp.exp(draws), shape[position] // blocks).reshape((-1,) + (1,) * (len(shape) - 1 - position))
    return loudness


def noise(stream_key, dims, spread, reach, pieces=(), kind=jnp.bfloat16):
    result = spread * jax.random.normal(stream_key, dims, jnp.float32)
    if pieces:
        result = result * shard_levels(stream_key, dims, pieces, -0.22, 0.18)
    return jnp.clip(result, -reach, reach).astype(kind)


def setup_inputs(seed: int = 0, part: int = 0) -> dict:
    arg_keys = jax.random.split(jax.random.key(seed), 10)
    own_keys = jax.random.split(jax.random.fold_in(arg_keys[9], part), 10)
    return {
        "tracer": noise(own_keys[0], (K, NLAT, NLON), 1.0, 6.0, ((1, 4), (2, 4)), jnp.float32),
        "velocity": noise(own_keys[1], (2, K, NLAT, NLON), 0.15, 0.9, ((2, 4), (3, 4)), jnp.float32),
        "surface": noise(own_keys[2], (NLAT, NLON), 1.0, 6.0, ((0, 4), (1, 4)), jnp.float32),
        "transport": noise(own_keys[3], (2, NLAT, NLON), 0.5, 3.0, ((1, 4), (2, 4)), jnp.float32),
        "horiz_mixing": jnp.clip(jnp.exp(jax.random.uniform(own_keys[4], (K,), jnp.float32, math.log(0.03), math.log(0.2))), 0.03, 0.2),
        "vert_mixing": jnp.clip(jnp.exp(jax.random.uniform(own_keys[5], (K - 1,), jnp.float32, math.log(0.3), math.log(30.0))), 0.3, 30.0),
        "levels": draw_levels(jax.random.fold_in(arg_keys[9], 71), part),
        "land_tiles": set_ends((jax.random.randint(arg_keys[7], (N_LAT, N_LON), 0, 4) < 1).astype(jnp.int32), jax.random.fold_in(arg_keys[7], 1), 0, 1),
        "fold_pair": draw_fold_pair(jax.random.fold_in(arg_keys[9], 71), part),
    }


fb_step = 0.6
drag_rate = 0.02


def east_of(field):
    return jnp.roll(field, -1, axis=-1)


def west_of(field):
    return jnp.roll(field, 1, axis=-1)


def north_of(field, fold_pair):
    top_row = jnp.take(field[..., -1:, :], fold_pair, axis=-1)
    return jnp.concatenate([field[..., 1:, :], top_row], axis=-2)


def south_of(field):
    return jnp.concatenate([jnp.zeros_like(field[..., :1, :]), field[..., :-1, :]], axis=-2)


def face_flux(near_side, far_side, wet_near, wet_far, vel_near, vel_far, mixing):
    return wet_near * wet_far * (mixing * (far_side - near_side) - 0.25 * (vel_near + vel_far) * (near_side + far_side))


def thomas(stepped, coupling):
    depth_count = stepped.shape[0]
    primes = []
    sweeps = []
    for depth_idx in range(depth_count):
        diagonal_term = jnp.ones_like(stepped[depth_idx])
        if depth_idx > 0:
            diagonal_term = diagonal_term + coupling[depth_idx - 1]
        if depth_idx < depth_count - 1:
            diagonal_term = diagonal_term + coupling[depth_idx]
        if depth_idx > 0:
            pivot_term = diagonal_term + coupling[depth_idx - 1] * primes[depth_idx - 1]
            reduced = (stepped[depth_idx] + coupling[depth_idx - 1] * sweeps[depth_idx - 1]) / pivot_term
        else:
            pivot_term = diagonal_term
            reduced = stepped[depth_idx] / pivot_term
        if depth_idx < depth_count - 1:
            primes.append(-coupling[depth_idx] / pivot_term)
        else:
            primes.append(jnp.zeros_like(reduced))
        sweeps.append(reduced)
    solved = [None] * depth_count
    solved[depth_count - 1] = sweeps[depth_count - 1]
    for depth_idx in range(depth_count - 2, -1, -1):
        solved[depth_idx] = sweeps[depth_idx] - primes[depth_idx] * solved[depth_idx + 1]
    return jnp.stack(solved)


def reference(tracer, velocity, surface, transport, horiz_mixing, vert_mixing, levels, land_tiles, fold_pair):
    tile_land = jnp.repeat(jnp.repeat(land_tiles, CLAT, axis=0), CLON, axis=1)
    depth_levels = (levels * (1 - tile_land)).astype(jnp.int32)
    level_real = depth_levels.astype(jnp.float32)
    sea_cells = (depth_levels > 0).astype(jnp.float32)
    wet = (jnp.arange(K, dtype=jnp.int32)[:, None, None] < depth_levels[None]).astype(jnp.float32)

    mixing = horiz_mixing[:, None, None]
    zonal_vel = velocity[0]
    merid_vel = velocity[1]
    flux_east = face_flux(tracer, east_of(tracer), wet, east_of(wet), zonal_vel, east_of(zonal_vel), mixing)
    flux_north = face_flux(tracer, north_of(tracer, fold_pair), wet, north_of(wet, fold_pair), merid_vel, north_of(merid_vel, fold_pair), mixing)
    stepped = wet * (tracer + ((flux_east - west_of(flux_east)) + (flux_north - south_of(flux_north))))
    coupling = vert_mixing[:, None, None] * wet[1:]
    tracer_new = thomas(stepped, coupling)

    zonal_mask = sea_cells * east_of(sea_cells)
    zonal_depth = (level_real + east_of(level_real)) / (2.0 * K)
    merid_mask = sea_cells * north_of(sea_cells, fold_pair)
    merid_depth = (level_real + north_of(level_real, fold_pair)) / (2.0 * K)

    height = surface
    zonal = transport[0]
    merid = transport[1]
    for substep in range(SUB):
        divergence = (zonal - west_of(zonal)) + (merid - south_of(merid))
        height = (height - fb_step * divergence) * sea_cells
        east_vals = east_of(height)
        north_vals = north_of(height, fold_pair)
        zonal = (zonal * (1.0 - drag_rate) - fb_step * zonal_depth * (east_vals - height)) * zonal_mask
        merid = (merid * (1.0 - drag_rate) - fb_step * merid_depth * (north_vals - height)) * merid_mask
    return tracer_new, height, jnp.stack([zonal, merid])
```

```python
import functools

import jax
import jax.numpy as jnp
from jax import lax
from jax.experimental import pallas as pl
from jax.experimental.pallas import tpu as pltpu
from jax.sharding import PartitionSpec as P

SUB = 12
LANES = 128
ROWS = 8

fb_step = 0.6
drag_rate = 0.02

E, W, N, S, NE, NW, SE, SW = range(8)


def lane_roll(field, shift):
    return pltpu.roll(field, shift % field.shape[1], 1)


def row_roll(field, shift):
    return pltpu.roll(field, shift % field.shape[0], 0)


def take_lanes(piece, idx):
    return jnp.take_along_axis(piece, idx, axis=1, mode="promise_in_bounds")


def kernel(
    n_lon,
    n_lat,
    tracer,
    velocity,
    surface,
    transport,
    horiz,
    vert,
    levels,
    land,
    fold_pair,
    tracer_new,
    surface_new,
    transport_new,
    nbuf,
    sbuf,
    ewbuf,
    from_n,
    from_s,
    from_e,
    from_w,
    corner,
    fold,
    north_b,
    diff_row,
    inv_pivot,
    primes,
    send_sem,
    recv_sem,
    fold_send,
    fold_recv,
):
    depth_count, tile_rows, tile_cols = tracer.shape
    halves = tile_rows // ROWS
    lon = lax.axis_index("lon")
    lat = lax.axis_index("lat")
    at_top = lat == n_lat - 1
    at_bottom = lat == 0
    east = lax.rem(lon + 1, n_lon)
    west = lax.rem(lon + n_lon - 1, n_lon)
    f32 = jnp.float32
    height_rows = 4 * tile_rows

    def place(lon_to, lat_to):
        return {"lon": lon_to, "lat": lat_to}

    barrier = pltpu.get_barrier_semaphore()

    def greet(lon_to, lat_to):
        pl.semaphore_signal(
            barrier, inc=1, device_id=place(lon_to, lat_to), device_id_type=pl.DeviceIdType.MESH
        )

    greet(east, lat)
    greet(west, lat)

    @pl.when(jnp.logical_not(at_top))
    def _():
        for other in (lon, east, west):
            greet(other, lat + 1)

    @pl.when(jnp.logical_not(at_bottom))
    def _():
        for other in (lon, east, west):
            greet(other, lat - 1)

    @pl.when(at_top)
    def _():
        for r in range(2, n_lon - 1):
            greet(lax.rem(lon + r, n_lon), lat)

    lane = lax.broadcasted_iota(jnp.int32, (ROWS, LANES), 1)
    sub = lax.broadcasted_iota(jnp.int32, (ROWS, LANES), 0)
    lane_t = lax.broadcasted_iota(jnp.int32, (tile_rows, LANES), 1)
    row_t = lax.broadcasted_iota(jnp.int32, (tile_rows, LANES), 0)

    depth = (levels[...] * (1 - land[0, 0])).astype(f32)
    own = [surface[...], transport[0], transport[1], depth]

    for f in range(4):
        sbuf[pl.ds(f * tile_rows, tile_rows), :] = own[f]
    sbuf[pl.ds(height_rows, depth_count), :] = tracer[:, 0, :]
    sbuf[pl.ds(height_rows + depth_count, depth_count), :] = velocity[1, :, 0, :]
    nbuf[pl.ds(height_rows, depth_count), :] = tracer[:, tile_rows - 1, :]
    nbuf[pl.ds(height_rows + depth_count, depth_count), :] = velocity[1, :, tile_rows - 1, :]

    @pl.when(jnp.logical_not(at_top))
    def _():
        for f in range(4):
            nbuf[pl.ds(f * tile_rows, tile_rows), :] = own[f]

    @pl.when(at_top)
    def _():
        for f in range(4):
            for k in range(tile_rows):
                row = tile_rows - 1 - k
                if f == 2:
                    row = row - 1 if row else tile_rows - 1
                value = sbuf[pl.ds(f * tile_rows + row, 1), :]
                if f == 1 or (f == 2 and k < tile_rows - 1):
                    value = -value
                nbuf[pl.ds(f * tile_rows + k, 1), :] = value

    slot = LANES // 4
    pack = jnp.zeros((tile_rows, LANES), f32)
    for f in range(4):
        pack = jnp.where(lane_t // slot == f, lane_roll(own[f], SUB + slot * f), pack)
    ewbuf[pl.ds(0, tile_rows), :] = pack

    pair_lane = lane // 2
    edge_t = jnp.zeros((ROWS, LANES), f32)
    edge_u = jnp.zeros((ROWS, LANES), f32)
    for k in range(depth_count):
        for r in range(halves):
            m = k * halves + r
            pick = pair_lane == m
            edge_t = jnp.where(pick, lane_roll(tracer[k, pl.ds(r * ROWS, ROWS), :], 2 * m + 1), edge_t)
            edge_u = jnp.where(
                pick, lane_roll(velocity[0, k, pl.ds(r * ROWS, ROWS), :], 2 * m + 1), edge_u
            )
    ewbuf[pl.ds(tile_rows, ROWS), :] = edge_t
    ewbuf[pl.ds(tile_rows + ROWS, ROWS), :] = edge_u

    @pl.when(at_bottom)
    def _():
        from_s[...] = jnp.zeros_like(from_s)
        corner[SE - NE] = jnp.zeros((tile_rows, LANES), f32)
        corner[SW - NE] = jnp.zeros((tile_rows, LANES), f32)

    top = (lat + 1) // n_lat
    bottom = (n_lat - lat) // n_lat
    pl.semaphore_wait(barrier, 2 + 3 * (1 - top) + 3 * (1 - bottom) + (n_lon - 3) * top)

    def copy(src, dst, to, came, lon_to, lat_to):
        return pltpu.make_async_remote_copy(
            src_ref=src,
            dst_ref=dst,
            send_sem=send_sem.at[to],
            recv_sem=recv_sem.at[came],
            device_id=place(lon_to, lat_to),
            device_id_type=pl.DeviceIdType.MESH,
        )

    tile_pack = ewbuf.at[pl.ds(0, tile_rows)]
    to_e = copy(ewbuf, from_w, E, W, east, lat)
    to_w = copy(ewbuf, from_e, W, E, west, lat)
    up = lat + 1
    down = lat - 1
    to_n = copy(nbuf, from_s, N, S, lon, up)
    to_ne = copy(tile_pack, corner.at[SW - NE], NE, SW, east, up)
    to_nw = copy(tile_pack, corner.at[SE - NE], NW, SE, west, up)
    to_s = copy(sbuf, from_n, S, N, lon, down)
    to_se = copy(tile_pack, corner.at[NW - NE], SE, NW, east, down)
    to_sw = copy(tile_pack, corner.at[NE - NE], SW, NE, west, down)
    to_fold = [
        pltpu.make_async_remote_copy(
            src_ref=nbuf,
            dst_ref=fold.at[r - 1],
            send_sem=fold_send.at[r - 1],
            recv_sem=fold_recv.at[r - 1],
            device_id=place(lax.rem(lon + r, n_lon), lat),
            device_id_type=pl.DeviceIdType.MESH,
        )
        for r in range(1, n_lon)
    ]

    @pl.when(at_top)
    def _():
        for one in to_fold:
            one.start()

    @pl.when(jnp.logical_not(at_top))
    def _():
        to_n.start()
        to_ne.start()
        to_nw.start()

    @pl.when(jnp.logical_not(at_bottom))
    def _():
        to_s.start()
        to_se.start()
        to_sw.start()

    to_e.start()
    to_w.start()

    prime = None
    for k in range(depth_count):
        diagonal = jnp.ones((tile_rows, LANES), f32)
        if k > 0:
            above = jnp.where(depth > k, vert[k - 1], 0.0)
            diagonal = diagonal + above
        if k < depth_count - 1:
            below = jnp.where(depth > k + 1, vert[k], 0.0)
            diagonal = diagonal + below
        if k > 0:
            diagonal = diagonal + above * prime
        inverse = 1.0 / diagonal
        inv_pivot[k] = inverse
        if k < depth_count - 1:
            prime = -below * inverse
            primes[k] = prime

    to_e.wait_recv()
    to_w.wait_recv()

    @pl.when(jnp.logical_not(at_bottom))
    def _():
        to_n.wait_recv()
        to_ne.wait_recv()
        to_nw.wait_recv()

    w_slot = lane_t % slot < SUB
    in_halo = jnp.logical_or(lane_t < SUB, lane_t >= LANES - SUB)
    deep_halo = jnp.logical_or(lane_t < SUB + 1, lane_t >= LANES - SUB)

    def side_tiles(e_pack, w_pack):
        both = jnp.where(w_slot, w_pack, e_pack)
        return [jnp.where(in_halo, lane_roll(both, -(slot * f + SUB)), 0.0) for f in range(4)]

    @pl.when(jnp.logical_not(at_top))
    def _():
        to_s.wait_recv()
        to_se.wait_recv()
        to_sw.wait_recv()
        for f, tile in enumerate(side_tiles(corner[NE - NE], corner[NW - NE])):
            north_b[pl.ds(f * tile_rows, tile_rows), :] = tile
        diff_row[...] = jnp.zeros_like(diff_row)

    @pl.when(at_top)
    def _():
        pair = jnp.broadcast_to(fold_pair[...], (ROWS, LANES))
        idx = pair % tile_cols
        tile_a = pair // tile_cols
        tile_b = jnp.where(
            lane < LANES // 2,
            jnp.where(tile_a == 0, n_lon - 1, tile_a - 1),
            jnp.where(tile_a == n_lon - 1, 0, tile_a + 1),
        )
        for one in to_fold:
            one.wait_recv()
        sources = [(nbuf, lon)]
        for r in range(1, n_lon):
            sources.append((fold.at[r - 1], lax.rem(lon + n_lon - r, n_lon)))

        def mirrored(start, with_b):
            part_a = jnp.zeros((ROWS, LANES), f32)
            part_b = jnp.zeros((ROWS, LANES), f32)
            for ref, which in sources:
                piece = take_lanes(ref[pl.ds(start, ROWS), :], idx)
                part_a = jnp.where(tile_a == which, piece, part_a)
                if with_b:
                    part_b = jnp.where(tile_b == which, piece, part_b)
            return part_a, part_b

        for f in range(4):
            for r in range(halves):
                start = f * tile_rows + r * ROWS
                part_a, part_b = mirrored(start, True)
                part_b = jnp.where(deep_halo[:ROWS], part_b, 0.0)
                if f == 1:
                    next_a = lane_roll(part_a, -1)
                    next_b = lane_roll(part_b, -1)
                    part_a = jnp.where(lane == LANES - 1, next_b, next_a)
                    part_b = jnp.where(lane == LANES - 1, next_a, next_b)
                if f == 2 and r == halves - 1:
                    across_a = row_roll(part_a, 1)
                    across_b = row_roll(part_b, 1)
                    own_a = sbuf[pl.ds(3 * tile_rows - 1, 1), :]
                    both = jnp.where(w_slot, from_w[pl.ds(0, tile_rows), :], from_e[pl.ds(0, tile_rows), :])
                    own_b = jnp.where(in_halo, lane_roll(both, -(slot * 2 + SUB)), 0.0)
                    own_b = row_roll(own_b, 1)[:ROWS]
                    diff_row[:, :LANES] = jnp.where(sub == 0, -(across_a + own_a), 0.0)
                    diff_row[:, LANES:] = jnp.where(sub == 0, -(across_b + own_b), 0.0)
                from_n[pl.ds(start, ROWS), :] = part_a
                north_b[pl.ds(start, ROWS), :] = part_b
        for q in range(2 * depth_count // ROWS):
            start = height_rows + q * ROWS
            from_n[pl.ds(start, ROWS), :] = mirrored(start, False)[0]

    own_b = side_tiles(from_e[pl.ds(0, tile_rows), :], from_w[pl.ds(0, tile_rows), :])
    south_b = side_tiles(corner[SE - NE], corner[SW - NE])
    full = SUB // ROWS
    rem = SUB % ROWS

    def ring(own_tile, north_tile, south_tile):
        pieces = [own_tile, north_tile[: full * ROWS]]
        if rem:
            pieces.append(
                jnp.where(
                    sub < rem,
                    north_tile[full * ROWS : (full + 1) * ROWS],
                    south_tile[tile_rows - (full + 1) * ROWS : tile_rows - full * ROWS],
                )
            )
        pieces.append(south_tile[tile_rows - full * ROWS :])
        return jnp.concatenate(pieces, axis=0)

    fields = []
    for f in range(4):
        rows = pl.ds(f * tile_rows, tile_rows)
        fields.append(
            jnp.concatenate(
                [
                    ring(own[f], from_n[rows, :], from_s[rows, :]),
                    ring(own_b[f], north_b[rows, :], south_b[f]),
                ],
                axis=1,
            )
        )
    height, zonal, merid, level_real = fields
    sea = jnp.where(level_real > 0, 1.0, 0.0)
    scale = fb_step / (2.0 * depth_count)
    zonal_mask = sea * lane_roll(sea, -1)
    merid_mask = sea * row_roll(sea, -1)
    zonal_fact = (level_real + lane_roll(level_real, -1)) * scale * zonal_mask
    merid_fact = (level_real + row_roll(level_real, -1)) * scale * merid_mask
    zonal_keep = zonal_mask * (1.0 - drag_rate)
    merid_keep = merid_mask * (1.0 - drag_rate)
    diff = diff_row[...]
    diff_keep = row_roll(merid_keep, 1)[tile_rows : tile_rows + ROWS]
    sea_step = sea * fb_step
    for _ in range(SUB):
        south_v = row_roll(merid, 1)
        south_v = jnp.concatenate(
            [
                south_v[:tile_rows],
                south_v[tile_rows : tile_rows + ROWS] + diff,
                south_v[tile_rows + ROWS :],
            ],
            axis=0,
        )
        diff = diff * diff_keep
        divergence = (zonal - lane_roll(zonal, 1)) + (merid - south_v)
        height = height * sea - sea_step * divergence
        zonal = zonal * zonal_keep - zonal_fact * (lane_roll(height, -1) - height)
        merid = merid * merid_keep - merid_fact * (row_roll(height, -1) - height)
    surface_new[...] = height[:tile_rows, :LANES]
    transport_new[0] = zonal[:tile_rows, :LANES]
    transport_new[1] = merid[:tile_rows, :LANES]

    def face(a, b, va, vb, mix):
        return mix * (b - a) - 0.25 * (va + vb) * (a + b)

    odd = lane % 2 == 1

    def swap(e_edge, w_edge):
        return jnp.where(odd, lane_roll(w_edge, 1), lane_roll(e_edge, -1))

    rows_t = pl.ds(tile_rows, ROWS)
    rows_u = pl.ds(tile_rows + ROWS, ROWS)
    far_t = swap(from_e[rows_t, :], from_w[rows_t, :])
    far_u = swap(from_e[rows_u, :], from_w[rows_u, :])
    level_lane = lane // (2 * halves)
    mix_pack = jnp.zeros((ROWS, LANES), f32)
    for k in range(depth_count):
        mix_pack = jnp.where(level_lane == k, horiz[k], mix_pack)
    own_level = jnp.zeros((ROWS, LANES), f32)
    far_level = jnp.zeros((ROWS, LANES), f32)
    half_lane = pair_lane % halves
    for r in range(halves):
        mine = depth[r * ROWS : (r + 1) * ROWS]
        beside = own_b[3][r * ROWS : (r + 1) * ROWS]
        own_level = jnp.where(
            half_lane == r, jnp.where(odd, mine[:, :1], mine[:, LANES - 1 :]), own_level
        )
        far_level = jnp.where(
            half_lane == r, jnp.where(odd, beside[:, LANES - 1 :], beside[:, :1]), far_level
        )
    level_f = level_lane.astype(f32)
    side_wet = jnp.logical_and(level_f < own_level, level_f < far_level)
    side_mix = jnp.where(odd, -mix_pack, mix_pack)
    side_flux = jnp.where(side_wet, face(edge_t, far_t, edge_u, far_u, side_mix), 0.0)

    k_col = lax.broadcasted_iota(jnp.int32, (depth_count, LANES), 0)
    k_real = k_col.astype(f32)
    mix_col = jnp.zeros((depth_count, LANES), f32)
    for k in range(depth_count):
        mix_col = jnp.where(k_col == k, horiz[k], mix_col)
    t_rows = pl.ds(height_rows, depth_count)
    v_rows = pl.ds(height_rows + depth_count, depth_count)
    north_level = from_n[pl.ds(3 * tile_rows, 1), :]
    south_level = from_s[pl.ds(4 * tile_rows - 1, 1), :]
    north_flux = jnp.where(
        jnp.logical_and(k_real < depth[tile_rows - 1 :], k_real < north_level),
        face(nbuf[t_rows, :], from_n[t_rows, :], nbuf[v_rows, :], from_n[v_rows, :], mix_col),
        0.0,
    )
    south_flux = jnp.where(
        jnp.logical_and(k_real < depth[:1], k_real < south_level),
        face(from_s[t_rows, :], sbuf[t_rows, :], from_s[v_rows, :], sbuf[v_rows, :], mix_col),
        0.0,
    )

    east_level = jnp.minimum(depth, lane_roll(depth, -1))
    up_level = jnp.minimum(depth, row_roll(depth, -1))
    sweep = None
    for k in range(depth_count):
        field = tracer[k]
        zonal_vel = velocity[0, k]
        merid_vel = velocity[1, k]
        side = jnp.concatenate(
            [lane_roll(side_flux, -(2 * (k * halves + r) + 1)) for r in range(halves)], axis=0
        )
        flux_e = face(field, lane_roll(field, -1), zonal_vel, lane_roll(zonal_vel, -1), horiz[k])
        flux_e = jnp.where(lane_t == LANES - 1, side, jnp.where(east_level > k, flux_e, 0.0))
        flux_w = jnp.where(lane_t == 0, side, lane_roll(flux_e, 1))
        flux_n = face(field, row_roll(field, -1), merid_vel, row_roll(merid_vel, -1), horiz[k])
        flux_n = jnp.where(
            row_t == tile_rows - 1, north_flux[k : k + 1], jnp.where(up_level > k, flux_n, 0.0)
        )
        flux_s = jnp.where(row_t == 0, south_flux[k : k + 1], row_roll(flux_n, 1))
        stepped = jnp.where(depth > k, field + ((flux_e - flux_w) + (flux_n - flux_s)), 0.0)
        if k > 0:
            above = jnp.where(depth > k, vert[k - 1], 0.0)
            stepped = stepped + above * sweep
        sweep = stepped * inv_pivot[k]
        tracer_new[k] = sweep
    solved = sweep
    for k in range(depth_count - 2, -1, -1):
        solved = tracer_new[k] - primes[k] * solved
        tracer_new[k] = solved

    to_e.wait_send()
    to_w.wait_send()

    @pl.when(jnp.logical_not(at_top))
    def _():
        to_n.wait_send()
        to_ne.wait_send()
        to_nw.wait_send()

    @pl.when(jnp.logical_not(at_bottom))
    def _():
        to_s.wait_send()
        to_se.wait_send()
        to_sw.wait_send()

    @pl.when(at_top)
    def _():
        for one in to_fold:
            one.wait_send()


def shards(
    n_lon,
    n_lat,
    tracer,
    velocity,
    surface,
    transport,
    horiz_mixing,
    vert_mixing,
    levels,
    land_tiles,
    fold_pair,
):
    depth_count, tile_rows, tile_cols = tracer.shape
    vmem = pl.BlockSpec(memory_space=pltpu.VMEM)
    smem = pl.BlockSpec(memory_space=pltpu.SMEM)
    f32 = jnp.float32
    message = 4 * tile_rows + 2 * depth_count
    return pl.pallas_call(
        functools.partial(kernel, n_lon, n_lat),
        out_shape=(
            jax.ShapeDtypeStruct(tracer.shape, f32),
            jax.ShapeDtypeStruct(surface.shape, f32),
            jax.ShapeDtypeStruct(transport.shape, f32),
        ),
        in_specs=[vmem, vmem, vmem, vmem, smem, smem, vmem, smem, vmem],
        out_specs=(vmem, vmem, vmem),
        scratch_shapes=[
            pltpu.VMEM((message, LANES), f32),
            pltpu.VMEM((message, LANES), f32),
            pltpu.VMEM((tile_rows + 2 * ROWS, LANES), f32),
            pltpu.VMEM((message, LANES), f32),
            pltpu.VMEM((message, LANES), f32),
            pltpu.VMEM((tile_rows + 2 * ROWS, LANES), f32),
            pltpu.VMEM((tile_rows + 2 * ROWS, LANES), f32),
            pltpu.VMEM((4, tile_rows, LANES), f32),
            pltpu.VMEM((n_lon - 1, message, LANES), f32),
            pltpu.VMEM((4 * tile_rows, LANES), f32),
            pltpu.VMEM((ROWS, 2 * LANES), f32),
            pltpu.VMEM(tracer.shape, f32),
            pltpu.VMEM(tracer.shape, f32),
            pltpu.SemaphoreType.DMA((8,)),
            pltpu.SemaphoreType.DMA((8,)),
            pltpu.SemaphoreType.DMA((n_lon - 1,)),
            pltpu.SemaphoreType.DMA((n_lon - 1,)),
        ],
        compiler_params=pltpu.CompilerParams(collective_id=0, has_side_effects=True),
    )(
        tracer,
        velocity,
        surface,
        transport,
        horiz_mixing,
        vert_mixing,
        levels,
        land_tiles,
        fold_pair[None],
    )


def solution(mesh):
    return jax.shard_map(
        functools.partial(shards, mesh.shape["lon"], mesh.shape["lat"]),
        mesh=mesh,
        in_specs=(
            P("member", "lat", "lon"),
            P(None, "member", "lat", "lon"),
            P(("member", "lat"), "lon"),
            P("member", "lat", "lon"),
            P("member"),
            P("member"),
            P("lat", "lon"),
            P("lat", "lon"),
            P("lon"),
        ),
        out_specs=(
            P("member", "lat", "lon"),
            P(("member", "lat"), "lon"),
            P("member", "lat", "lon"),
        ),
        check_vma=False,
    )
```

```python
import functools

import jax
import jax.numpy as jnp
from jax import lax
from jax.experimental import pallas as pl
from jax.experimental.pallas import tpu as pltpu
from jax.sharding import PartitionSpec as P

SUB = 12
LANES = 128
ROWS = 8

fb_step = 0.6
drag_rate = 0.02

E, W, N, S, NE, NW, SE, SW, E2, W2, N2, S2 = range(12)


def lane_roll(field, shift):
    return pltpu.roll(field, shift % field.shape[1], 1)


def row_roll(field, shift):
    return pltpu.roll(field, shift % field.shape[0], 0)


def take_lanes(piece, idx):
    return jnp.take_along_axis(piece, idx, axis=1, mode="promise_in_bounds")


def kernel(
    n_lon,
    n_lat,
    tracer_in,
    velocity_in,
    surface_in,
    transport_in,
    horiz_in,
    vert_in,
    levels_in,
    land_in,
    fold_pair_in,
    sweeps,
    primes,
    surface_new,
    transport_new,
    tracer,
    velocity,
    surface,
    transport,
    levels,
    fold_pair,
    horiz,
    vert,
    land,
    inner,
    nbuf,
    sbuf,
    ewbuf,
    from_n,
    from_s,
    from_e,
    from_w,
    corner,
    fold,
    north_b,
    diff_row,
    inv_pivot,
    in_sem,
    send_sem,
    recv_sem,
    fold_send,
    fold_recv,
):
    depth_count, tile_rows, tile_cols = tracer.shape
    halves = tile_rows // ROWS
    lon = lax.axis_index("lon")
    lat = lax.axis_index("lat")
    at_top = lat == n_lat - 1
    at_bottom = lat == 0
    east = lax.rem(lon + 1, n_lon)
    west = lax.rem(lon + n_lon - 1, n_lon)
    f32 = jnp.float32
    height_rows = 4 * tile_rows

    def place(lon_to, lat_to):
        return {"lon": lon_to, "lat": lat_to}

    pairs = [
        (levels_in, levels),
        (land_in, land),
        (surface_in, surface),
        (transport_in, transport),
        (tracer_in, tracer),
        (velocity_in, velocity),
        (fold_pair_in, fold_pair),
        (horiz_in, horiz),
        (vert_in, vert),
    ]
    loads = [pltpu.make_async_copy(a, b, in_sem.at[i]) for i, (a, b) in enumerate(pairs)]
    for load in loads:
        load.start()

    barrier = pltpu.get_barrier_semaphore()

    def greet(lon_to, lat_to):
        pl.semaphore_signal(
            barrier, inc=1, device_id=place(lon_to, lat_to), device_id_type=pl.DeviceIdType.MESH
        )

    greet(east, lat)
    greet(west, lat)

    @pl.when(jnp.logical_not(at_top))
    def _():
        for other in (lon, east, west):
            greet(other, lat + 1)

    @pl.when(jnp.logical_not(at_bottom))
    def _():
        for other in (lon, east, west):
            greet(other, lat - 1)

    @pl.when(at_top)
    def _():
        for r in range(2, n_lon - 1):
            greet(lax.rem(lon + r, n_lon), lat)

    lane = lax.broadcasted_iota(jnp.int32, (ROWS, LANES), 1)
    sub = lax.broadcasted_iota(jnp.int32, (ROWS, LANES), 0)
    lane_t = lax.broadcasted_iota(jnp.int32, (tile_rows, LANES), 1)
    row_t = lax.broadcasted_iota(jnp.int32, (tile_rows, LANES), 0)

    for load in loads[:4]:
        load.wait()
    depth = (levels[...] * (1 - land[0, 0])).astype(f32)
    own = [surface[...], transport[0], transport[1], depth]

    for f in range(4):
        sbuf[pl.ds(f * tile_rows, tile_rows), :] = own[f]

    @pl.when(jnp.logical_not(at_top))
    def _():
        for f in range(4):
            nbuf[pl.ds(f * tile_rows, tile_rows), :] = own[f]

    @pl.when(at_top)
    def _():
        for f in range(4):
            for k in range(tile_rows):
                row = tile_rows - 1 - k
                if f == 2:
                    row = row - 1 if row else tile_rows - 1
                value = sbuf[pl.ds(f * tile_rows + row, 1), :]
                if f == 1 or (f == 2 and k < tile_rows - 1):
                    value = -value
                nbuf[pl.ds(f * tile_rows + k, 1), :] = value

    slot = LANES // 4
    pack = jnp.zeros((tile_rows, LANES), f32)
    for f in range(4):
        pack = jnp.where(lane_t // slot == f, lane_roll(own[f], SUB + slot * f), pack)
    ewbuf[pl.ds(0, tile_rows), :] = pack

    @pl.when(at_bottom)
    def _():
        from_s[...] = jnp.zeros_like(from_s)
        corner[SE - NE] = jnp.zeros((tile_rows, LANES), f32)
        corner[SW - NE] = jnp.zeros((tile_rows, LANES), f32)

    top = (lat + 1) // n_lat
    bottom = (n_lat - lat) // n_lat
    pl.semaphore_wait(barrier, 2 + 3 * (1 - top) + 3 * (1 - bottom) + (n_lon - 3) * top)

    def copy(src, dst, to, came, lon_to, lat_to):
        return pltpu.make_async_remote_copy(
            src_ref=src,
            dst_ref=dst,
            send_sem=send_sem.at[to],
            recv_sem=recv_sem.at[came],
            device_id=place(lon_to, lat_to),
            device_id_type=pl.DeviceIdType.MESH,
        )

    tile_pack = ewbuf.at[pl.ds(0, tile_rows)]
    edges = pl.ds(tile_rows, 2 * ROWS)
    first = pl.ds(0, height_rows)
    later = pl.ds(height_rows, 2 * depth_count)
    up = lat + 1
    down = lat - 1
    to_e = copy(tile_pack, from_w.at[pl.ds(0, tile_rows)], E, W, east, lat)
    to_w = copy(tile_pack, from_e.at[pl.ds(0, tile_rows)], W, E, west, lat)
    to_e2 = copy(ewbuf.at[edges], from_w.at[edges], E2, W2, east, lat)
    to_w2 = copy(ewbuf.at[edges], from_e.at[edges], W2, E2, west, lat)
    to_n = copy(nbuf.at[first], from_s.at[first], N, S, lon, up)
    to_n2 = copy(nbuf.at[later], from_s.at[later], N2, S2, lon, up)
    to_ne = copy(tile_pack, corner.at[SW - NE], NE, SW, east, up)
    to_nw = copy(tile_pack, corner.at[SE - NE], NW, SE, west, up)
    to_s = copy(sbuf.at[first], from_n.at[first], S, N, lon, down)
    to_s2 = copy(sbuf.at[later], from_n.at[later], S2, N2, lon, down)
    to_se = copy(tile_pack, corner.at[NW - NE], SE, NW, east, down)
    to_sw = copy(tile_pack, corner.at[NE - NE], SW, NE, west, down)

    def around(part, base):
        return [
            pltpu.make_async_remote_copy(
                src_ref=nbuf.at[part],
                dst_ref=fold.at[r - 1, part],
                send_sem=fold_send.at[base + r - 1],
                recv_sem=fold_recv.at[base + r - 1],
                device_id=place(lax.rem(lon + r, n_lon), lat),
                device_id_type=pl.DeviceIdType.MESH,
            )
            for r in range(1, n_lon)
        ]

    to_fold = around(first, 0)
    to_fold2 = around(later, n_lon - 1)

    @pl.when(at_top)
    def _():
        for one in to_fold:
            one.start()

    @pl.when(jnp.logical_not(at_top))
    def _():
        to_n.start()
        to_ne.start()
        to_nw.start()

    @pl.when(jnp.logical_not(at_bottom))
    def _():
        to_s.start()
        to_se.start()
        to_sw.start()

    to_e.start()
    to_w.start()

    for load in loads[4:]:
        load.wait()
    sbuf[pl.ds(height_rows, depth_count), :] = tracer[:, 0, :]
    sbuf[pl.ds(height_rows + depth_count, depth_count), :] = velocity[1, :, 0, :]
    nbuf[pl.ds(height_rows, depth_count), :] = tracer[:, tile_rows - 1, :]
    nbuf[pl.ds(height_rows + depth_count, depth_count), :] = velocity[1, :, tile_rows - 1, :]


    pair_lane = lane // 2
    edge_t = jnp.zeros((ROWS, LANES), f32)
    edge_u = jnp.zeros((ROWS, LANES), f32)
    for k in range(depth_count):
        for r in range(halves):
            m = k * halves + r
            pick = pair_lane == m
            edge_t = jnp.where(pick, lane_roll(tracer[k, pl.ds(r * ROWS, ROWS), :], 2 * m + 1), edge_t)
            edge_u = jnp.where(
                pick, lane_roll(velocity[0, k, pl.ds(r * ROWS, ROWS), :], 2 * m + 1), edge_u
            )
    ewbuf[pl.ds(tile_rows, ROWS), :] = edge_t
    ewbuf[pl.ds(tile_rows + ROWS, ROWS), :] = edge_u


    @pl.when(at_top)
    def _():
        for one in to_fold2:
            one.start()

    @pl.when(jnp.logical_not(at_top))
    def _():
        to_n2.start()

    @pl.when(jnp.logical_not(at_bottom))
    def _():
        to_s2.start()

    to_e2.start()
    to_w2.start()

    def face(a, b, va, vb, mix):
        return mix * (b - a) - 0.25 * (va + vb) * (a + b)

    east_level = jnp.where(lane_t == LANES - 1, 0.0, jnp.minimum(depth, lane_roll(depth, -1)))
    up_level = jnp.where(row_t == tile_rows - 1, 0.0, jnp.minimum(depth, row_roll(depth, -1)))
    for k in range(depth_count):
        field = tracer[k]
        zonal_vel = velocity[0, k]
        merid_vel = velocity[1, k]
        flux_e = face(field, lane_roll(field, -1), zonal_vel, lane_roll(zonal_vel, -1), horiz[k])
        flux_e = jnp.where(east_level > k, flux_e, 0.0)
        flux_n = face(field, row_roll(field, -1), merid_vel, row_roll(merid_vel, -1), horiz[k])
        flux_n = jnp.where(up_level > k, flux_n, 0.0)
        inner[k] = field + ((flux_e - lane_roll(flux_e, 1)) + (flux_n - row_roll(flux_n, 1)))

    prime = None
    for k in range(depth_count):
        diagonal = jnp.ones((tile_rows, LANES), f32)
        if k > 0:
            above = jnp.where(depth > k, vert[k - 1], 0.0)
            diagonal = diagonal + above
        if k < depth_count - 1:
            below = jnp.where(depth > k + 1, vert[k], 0.0)
            diagonal = diagonal + below
        if k > 0:
            diagonal = diagonal + above * prime
        inverse = 1.0 / diagonal
        inv_pivot[k] = inverse
        if k < depth_count - 1:
            prime = -below * inverse
            primes[k] = prime
    primes[depth_count - 1] = jnp.zeros((tile_rows, LANES), f32)

    to_e.wait_recv()
    to_w.wait_recv()

    @pl.when(jnp.logical_not(at_bottom))
    def _():
        to_n.wait_recv()
        to_ne.wait_recv()
        to_nw.wait_recv()

    w_slot = lane_t % slot < SUB
    in_halo = jnp.logical_or(lane_t < SUB, lane_t >= LANES - SUB)
    deep_halo = jnp.logical_or(lane_t < SUB + 1, lane_t >= LANES - SUB)

    def side_tiles(e_pack, w_pack):
        both = jnp.where(w_slot, w_pack, e_pack)
        return [jnp.where(in_halo, lane_roll(both, -(slot * f + SUB)), 0.0) for f in range(4)]

    @pl.when(jnp.logical_not(at_top))
    def _():
        to_s.wait_recv()
        to_se.wait_recv()
        to_sw.wait_recv()
        for f, tile in enumerate(side_tiles(corner[NE - NE], corner[NW - NE])):
            north_b[pl.ds(f * tile_rows, tile_rows), :] = tile
        diff_row[...] = jnp.zeros_like(diff_row)

    sources = [(nbuf, lon)]
    for r in range(1, n_lon):
        sources.append((fold.at[r - 1], lax.rem(lon + n_lon - r, n_lon)))
    pair = jnp.broadcast_to(fold_pair[...], (ROWS, LANES))
    idx = pair % tile_cols
    tile_a = pair // tile_cols
    tile_b = jnp.where(
        lane < LANES // 2,
        jnp.where(tile_a == 0, n_lon - 1, tile_a - 1),
        jnp.where(tile_a == n_lon - 1, 0, tile_a + 1),
    )

    def mirrored(start, with_b):
        part_a = jnp.zeros((ROWS, LANES), f32)
        part_b = jnp.zeros((ROWS, LANES), f32)
        for ref, which in sources:
            piece = take_lanes(ref[pl.ds(start, ROWS), :], idx)
            part_a = jnp.where(tile_a == which, piece, part_a)
            if with_b:
                part_b = jnp.where(tile_b == which, piece, part_b)
        return part_a, part_b

    @pl.when(at_top)
    def _():
        for one in to_fold:
            one.wait_recv()
        for f in range(4):
            for r in range(halves):
                start = f * tile_rows + r * ROWS
                part_a, part_b = mirrored(start, True)
                part_b = jnp.where(deep_halo[:ROWS], part_b, 0.0)
                if f == 1:
                    next_a = lane_roll(part_a, -1)
                    next_b = lane_roll(part_b, -1)
                    part_a = jnp.where(lane == LANES - 1, next_b, next_a)
                    part_b = jnp.where(lane == LANES - 1, next_a, next_b)
                if f == 2 and r == halves - 1:
                    across_a = row_roll(part_a, 1)
                    across_b = row_roll(part_b, 1)
                    own_a = sbuf[pl.ds(3 * tile_rows - 1, 1), :]
                    both = jnp.where(w_slot, from_w[pl.ds(0, tile_rows), :], from_e[pl.ds(0, tile_rows), :])
                    own_b = jnp.where(in_halo, lane_roll(both, -(slot * 2 + SUB)), 0.0)
                    own_b = row_roll(own_b, 1)[:ROWS]
                    diff_row[:, :LANES] = jnp.where(sub == 0, -(across_a + own_a), 0.0)
                    diff_row[:, LANES:] = jnp.where(sub == 0, -(across_b + own_b), 0.0)
                from_n[pl.ds(start, ROWS), :] = part_a
                north_b[pl.ds(start, ROWS), :] = part_b
    own_b = side_tiles(from_e[pl.ds(0, tile_rows), :], from_w[pl.ds(0, tile_rows), :])
    south_b = side_tiles(corner[SE - NE], corner[SW - NE])
    full = SUB // ROWS
    rem = SUB % ROWS

    def ring(own_tile, north_tile, south_tile):
        pieces = [own_tile, north_tile[: full * ROWS]]
        if rem:
            pieces.append(
                jnp.where(
                    sub < rem,
                    north_tile[full * ROWS : (full + 1) * ROWS],
                    south_tile[tile_rows - (full + 1) * ROWS : tile_rows - full * ROWS],
                )
            )
        pieces.append(south_tile[tile_rows - full * ROWS :])
        return jnp.concatenate(pieces, axis=0)

    fields = []
    for f in range(4):
        rows = pl.ds(f * tile_rows, tile_rows)
        fields.append(
            jnp.concatenate(
                [
                    ring(own[f], from_n[rows, :], from_s[rows, :]),
                    ring(own_b[f], north_b[rows, :], south_b[f]),
                ],
                axis=1,
            )
        )
    height, zonal, merid, level_real = fields
    sea = jnp.where(level_real > 0, 1.0, 0.0)
    scale = fb_step / (2.0 * depth_count)
    zonal_mask = sea * lane_roll(sea, -1)
    merid_mask = sea * row_roll(sea, -1)
    zonal_fact = (level_real + lane_roll(level_real, -1)) * scale * zonal_mask
    merid_fact = (level_real + row_roll(level_real, -1)) * scale * merid_mask
    zonal_keep = zonal_mask * (1.0 - drag_rate)
    merid_keep = merid_mask * (1.0 - drag_rate)
    diff = diff_row[...]
    diff_keep = row_roll(merid_keep, 1)[tile_rows : tile_rows + ROWS]
    sea_step = sea * fb_step
    for _ in range(SUB):
        south_v = row_roll(merid, 1)
        south_v = jnp.concatenate(
            [
                south_v[:tile_rows],
                south_v[tile_rows : tile_rows + ROWS] + diff,
                south_v[tile_rows + ROWS :],
            ],
            axis=0,
        )
        diff = diff * diff_keep
        divergence = (zonal - lane_roll(zonal, 1)) + (merid - south_v)
        height = height * sea - sea_step * divergence
        zonal = zonal * zonal_keep - zonal_fact * (lane_roll(height, -1) - height)
        merid = merid * merid_keep - merid_fact * (row_roll(height, -1) - height)
    surface_new[...] = height[:tile_rows, :LANES]
    transport_new[0] = zonal[:tile_rows, :LANES]
    transport_new[1] = merid[:tile_rows, :LANES]

    to_e2.wait_recv()
    to_w2.wait_recv()

    @pl.when(jnp.logical_not(at_bottom))
    def _():
        to_n2.wait_recv()

    @pl.when(jnp.logical_not(at_top))
    def _():
        to_s2.wait_recv()

    @pl.when(at_top)
    def _():
        for one in to_fold2:
            one.wait_recv()
        for q in range(2 * depth_count // ROWS):
            start = height_rows + q * ROWS
            from_n[pl.ds(start, ROWS), :] = mirrored(start, False)[0]

    odd = lane % 2 == 1

    def swap(e_edge, w_edge):
        return jnp.where(odd, lane_roll(w_edge, 1), lane_roll(e_edge, -1))

    rows_t = pl.ds(tile_rows, ROWS)
    rows_u = pl.ds(tile_rows + ROWS, ROWS)
    far_t = swap(from_e[rows_t, :], from_w[rows_t, :])
    far_u = swap(from_e[rows_u, :], from_w[rows_u, :])
    level_lane = lane // (2 * halves)
    mix_pack = jnp.zeros((ROWS, LANES), f32)
    for k in range(depth_count):
        mix_pack = jnp.where(level_lane == k, horiz[k], mix_pack)
    own_level = jnp.zeros((ROWS, LANES), f32)
    far_level = jnp.zeros((ROWS, LANES), f32)
    half_lane = pair_lane % halves
    for r in range(halves):
        mine = depth[r * ROWS : (r + 1) * ROWS]
        beside = own_b[3][r * ROWS : (r + 1) * ROWS]
        own_level = jnp.where(
            half_lane == r, jnp.where(odd, mine[:, :1], mine[:, LANES - 1 :]), own_level
        )
        far_level = jnp.where(
            half_lane == r, jnp.where(odd, beside[:, LANES - 1 :], beside[:, :1]), far_level
        )
    level_f = level_lane.astype(f32)
    side_wet = jnp.logical_and(level_f < own_level, level_f < far_level)
    side_mix = jnp.where(odd, -mix_pack, mix_pack)
    side_flux = jnp.where(side_wet, face(edge_t, far_t, edge_u, far_u, side_mix), 0.0)
    side_flux = jnp.where(odd, -side_flux, side_flux)

    k_col = lax.broadcasted_iota(jnp.int32, (depth_count, LANES), 0)
    k_real = k_col.astype(f32)
    mix_col = jnp.zeros((depth_count, LANES), f32)
    for k in range(depth_count):
        mix_col = jnp.where(k_col == k, horiz[k], mix_col)
    t_rows = pl.ds(height_rows, depth_count)
    v_rows = pl.ds(height_rows + depth_count, depth_count)
    north_level = from_n[pl.ds(3 * tile_rows, 1), :]
    south_level = from_s[pl.ds(4 * tile_rows - 1, 1), :]
    north_flux = jnp.where(
        jnp.logical_and(k_real < depth[tile_rows - 1 :], k_real < north_level),
        face(nbuf[t_rows, :], from_n[t_rows, :], nbuf[v_rows, :], from_n[v_rows, :], mix_col),
        0.0,
    )
    south_flux = jnp.where(
        jnp.logical_and(k_real < depth[:1], k_real < south_level),
        face(from_s[t_rows, :], sbuf[t_rows, :], from_s[v_rows, :], sbuf[v_rows, :], mix_col),
        0.0,
    )

    rim = jnp.logical_or(lane_t == 0, lane_t == LANES - 1)
    sweep = None
    for k in range(depth_count):
        side = jnp.concatenate(
            [lane_roll(side_flux, -(2 * (k * halves + r) + 1)) for r in range(halves)], axis=0
        )
        ends = jnp.where(
            row_t == tile_rows - 1,
            north_flux[k : k + 1],
            jnp.where(row_t == 0, -south_flux[k : k + 1], 0.0),
        )
        stepped = inner[k] + (jnp.where(rim, side, 0.0) + ends)
        stepped = jnp.where(depth > k, stepped, 0.0)
        if k > 0:
            above = jnp.where(depth > k, vert[k - 1], 0.0)
            stepped = stepped + above * sweep
        sweep = stepped * inv_pivot[k]
        sweeps[k] = sweep

    to_e.wait_send()
    to_w.wait_send()
    to_e2.wait_send()
    to_w2.wait_send()

    @pl.when(jnp.logical_not(at_top))
    def _():
        to_n.wait_send()
        to_n2.wait_send()
        to_ne.wait_send()
        to_nw.wait_send()

    @pl.when(jnp.logical_not(at_bottom))
    def _():
        to_s.wait_send()
        to_s2.wait_send()
        to_se.wait_send()
        to_sw.wait_send()

    @pl.when(at_top)
    def _():
        for one in to_fold + to_fold2:
            one.wait_send()


CHUNK = 8


def finish(sweeps, primes, surface, transport, tracer_out, surface_out, transport_out, solution_buf, sem):
    depth_count = sweeps.shape[0]
    copies = [
        pltpu.make_async_copy(surface, surface_out, sem.at[0]),
        pltpu.make_async_copy(transport, transport_out, sem.at[1]),
    ]
    for one in copies:
        one.start()
    solved = None
    for k in range(depth_count - 1, -1, -1):
        solved = sweeps[k] if solved is None else sweeps[k] - primes[k] * solved
        solution_buf[k] = solved
        if k % CHUNK == 0:
            part = pl.ds(k, min(CHUNK, depth_count - k))
            one = pltpu.make_async_copy(
                solution_buf.at[part], tracer_out.at[part], sem.at[2 + k // CHUNK]
            )
            one.start()
            copies.append(one)
    for one in copies:
        one.wait()


def shards(
    n_lon,
    n_lat,
    tracer,
    velocity,
    surface,
    transport,
    horiz_mixing,
    vert_mixing,
    levels,
    land_tiles,
    fold_pair,
):
    depth_count, tile_rows, tile_cols = tracer.shape
    vmem = pl.BlockSpec(memory_space=pltpu.VMEM)
    f32 = jnp.float32
    message = 4 * tile_rows + 2 * depth_count
    held = pl.BlockSpec(memory_space=pltpu.HBM)
    sweeps, primes, height, flow = pl.pallas_call(
        functools.partial(kernel, n_lon, n_lat),
        out_shape=(
            pltpu.VMEM(tracer.shape, f32),
            pltpu.VMEM(tracer.shape, f32),
            pltpu.VMEM(surface.shape, f32),
            pltpu.VMEM(transport.shape, f32),
        ),
        in_specs=[held] * 9,
        out_specs=(vmem,) * 4,
        scratch_shapes=[
            pltpu.VMEM(tracer.shape, f32),
            pltpu.VMEM(velocity.shape, f32),
            pltpu.VMEM(surface.shape, f32),
            pltpu.VMEM(transport.shape, f32),
            pltpu.VMEM(levels.shape, jnp.int32),
            pltpu.VMEM((1, tile_cols), jnp.int32),
            pltpu.SMEM(horiz_mixing.shape, f32),
            pltpu.SMEM(vert_mixing.shape, f32),
            pltpu.SMEM((1, 1), jnp.int32),
            pltpu.VMEM(tracer.shape, f32),
            pltpu.VMEM((message, LANES), f32),
            pltpu.VMEM((message, LANES), f32),
            pltpu.VMEM((tile_rows + 2 * ROWS, LANES), f32),
            pltpu.VMEM((message, LANES), f32),
            pltpu.VMEM((message, LANES), f32),
            pltpu.VMEM((tile_rows + 2 * ROWS, LANES), f32),
            pltpu.VMEM((tile_rows + 2 * ROWS, LANES), f32),
            pltpu.VMEM((4, tile_rows, LANES), f32),
            pltpu.VMEM((n_lon - 1, message, LANES), f32),
            pltpu.VMEM((4 * tile_rows, LANES), f32),
            pltpu.VMEM((ROWS, 2 * LANES), f32),
            pltpu.VMEM(tracer.shape, f32),
            pltpu.SemaphoreType.DMA((9,)),
            pltpu.SemaphoreType.DMA((12,)),
            pltpu.SemaphoreType.DMA((12,)),
            pltpu.SemaphoreType.DMA((2 * (n_lon - 1),)),
            pltpu.SemaphoreType.DMA((2 * (n_lon - 1),)),
        ],
        compiler_params=pltpu.CompilerParams(collective_id=0, has_side_effects=True),
    )(
        tracer,
        velocity,
        surface,
        transport,
        horiz_mixing,
        vert_mixing,
        levels,
        land_tiles,
        fold_pair[None],
    )
    return pl.pallas_call(
        finish,
        out_shape=(
            jax.ShapeDtypeStruct(tracer.shape, f32),
            jax.ShapeDtypeStruct(surface.shape, f32),
            jax.ShapeDtypeStruct(transport.shape, f32),
        ),
        in_specs=[vmem] * 4,
        out_specs=(held,) * 3,
        scratch_shapes=[
            pltpu.VMEM(tracer.shape, f32),
            pltpu.SemaphoreType.DMA((2 + pl.cdiv(depth_count, CHUNK),)),
        ],
    )(*(pltpu.with_memory_space_constraint(x, pltpu.VMEM) for x in (sweeps, primes, height, flow)))


def solution(mesh):
    return jax.shard_map(
        functools.partial(shards, mesh.shape["lon"], mesh.shape["lat"]),
        mesh=mesh,
        in_specs=(
            P("member", "lat", "lon"),
            P(None, "member", "lat", "lon"),
            P(("member", "lat"), "lon"),
            P("member", "lat", "lon"),
            P("member"),
            P("member"),
            P("lat", "lon"),
            P("lat", "lon"),
            P("lon"),
        ),
        out_specs=(
            P("member", "lat", "lon"),
            P(("member", "lat"), "lon"),
            P("member", "lat", "lon"),
        ),
        check_vma=False,
    )
```
